32 devices in a mesh: dp: 8 (over y, x, core), tensor: 4 (over z).
Axes of the slice: x: 2, y: 2, z: 4, core: 2. Of those that a mesh axis runs over, the one named last changes fastest.
Arguments:
- tokens: bfloat16 [4096, 2048], P(('dp', 'tensor')), may hold values from -6 to 6
- query_weight: bfloat16 [2048, 2048], P(None, 'tensor'), may hold values from -2 to 2
- key_weight: bfloat16 [2048, 2048], P(None, 'tensor'), may hold values from -2 to 2
- value_weight: bfloat16 [2048, 2048], P(None, 'tensor'), may hold values from -0.125 to 0.125
- query_gain: float32 [16, 128], P('tensor'), may hold values from 0.5 to 4.6
- key_gain: float32 [16, 128], P('tensor'), may hold values from 0.5 to 4.6
- out_weight: bfloat16 [2048, 2048], P('tensor'), may hold values from -0.125 to 0.125
- attn_gain: float32 [2048], replicated, may hold values from 0.5 to 1.5
- gate_weight: bfloat16 [2048, 8192], P(None, 'tensor'), may hold values from -0.125 to 0.125
- up_weight: bfloat16 [2048, 8192], P(None, 'tensor'), may hold values from -0.125 to 0.125
- down_weight: bfloat16 [8192, 2048], P('tensor'), may hold values from -0.0625 to 0.0625
- mlp_gain: float32 [2048], replicated, may hold values from 0.5 to 1.5
- cotangent: float32 [4096, 2048], P(('dp', 'tensor')), may hold values from -6 to 6
Outputs:
- output: float32 [4096, 2048], P(('dp', 'tensor'))
- input_grad: float32 [4096, 2048], P(('dp', 'tensor'))
- grad_query_weight: float32 [2048, 2048], P('dp', 'tensor')
- grad_key_weight: float32 [2048, 2048], P('dp', 'tensor')
- grad_value_weight: float32 [2048, 2048], P('dp', 'tensor')
- grad_query_gain: float32 [16, 128], P('tensor', 'dp')
- grad_key_gain: float32 [16, 128], P('tensor', 'dp')
- grad_out_weight: float32 [2048, 2048], P('tensor', 'dp')
- grad_attn_gain: float32 [2048], P(('dp', 'tensor'))
- grad_gate_weight: float32 [2048, 8192], P('dp', 'tensor')
- grad_up_weight: float32 [2048, 8192], P('dp', 'tensor')
- grad_down_weight: float32 [8192, 2048], P('tensor', 'dp')
- grad_mlp_gain: float32 [2048], P(('dp', 'tensor'))
The draws below stay inside these ranges and needn't reach their ends.
All inputs are finite; a program needn't handle non-finite values.
Results may differ from the reference program's by a relative error of at most 0.018.
Values may be sent and summed in bfloat16 or wider, within the bound.
A program may use at most 256 MiB of HBM per device.

```python
import math
import jax
import jax.numpy as jnp
from jax import lax

D = 2048
H = 16
HD = 128
FF = 8192
L = 256
TOKENS = 4096


def gain_table(key, salt):
    return jnp.exp(jax.random.uniform(jax.random.fold_in(key, salt), (H, HD), jnp.float32, math.log(0.5), math.log(3.0)))


def draw_tokens(key, part):
    drawn_draw = jnp.clip(jax.random.normal(jax.random.fold_in(key, 21), (TOKENS, D), jnp.float32), -6.0, 6.0)
    return drawn_draw.astype(jnp.bfloat16)


def draw_query_weight(key, part):
    drawn_draw = jax.random.normal(jax.random.fold_in(key, 11), (D, D), jnp.float32) / math.sqrt(D)
    return drawn_draw.astype(jnp.bfloat16)


def draw_key_weight(key, part):
    drawn_draw = jax.random.normal(jax.random.fold_in(key, 12), (D, D), jnp.float32) / math.sqrt(D)
    return drawn_draw.astype(jnp.bfloat16)


def draw_query_gain(key, part):
    drawn_draw = gain_table(key, 31)
    return drawn_draw


def draw_key_gain(key, part):
    drawn_draw = gain_table(key, 41)
    return drawn_draw


def block_levels(key, shape, split, low, high):
    level = 1.0
    for dim, blocks in split:
        draws = jax.random.uniform(jax.random.fold_in(jax.random.fold_in(key, 6), dim), (blocks,), jnp.float32, low / len(split), high / len(split))
        level = level * jnp.repeat(jnp.exp(draws), shape[dim] // blocks).reshape((-1,) + (1,) * (len(shape) - 1 - dim))
    return level


def normal_values(key, extent, scale, reach, split=(), held_as=jnp.bfloat16):
    gain = block_levels(key, extent, split, -0.22, 0.18) if split else 1.0
    result = jax.random.normal(key, extent, jnp.float32) * scale * gain
    return jnp.minimum(jnp.maximum(result, -reach), reach).astype(held_as)


def setup_inputs(seed: int = 0) -> dict:
    key_list = jax.random.split(jax.random.key(seed), 14)
    tokens = draw_tokens(jax.random.fold_in(key_list[13], 71), 0)
    query_weight = draw_query_weight(jax.random.fold_in(key_list[13], 71), 0)
    key_weight = draw_key_weight(jax.random.fold_in(key_list[13], 71), 0)
    value_weight = normal_values(key_list[3], (D, D), D ** -0.5, 0.125, ((1, 4),))
    query_gain = draw_query_gain(jax.random.fold_in(key_list[13], 71), 0)
    key_gain = draw_key_gain(jax.random.fold_in(key_list[13], 71), 0)
    out_weight = normal_values(key_list[6], (D, D), D ** -0.5, 0.125, ((0, 4),))
    attn_gain = jnp.clip(1.0 + 0.1 * jax.random.normal(key_list[7], (D,), jnp.float32), 0.5, 1.5)
    gate_weight = normal_values(key_list[8], (D, FF), D ** -0.5, 0.125, ((1, 4),))
    up_weight = normal_values(key_list[9], (D, FF), D ** -0.5, 0.125, ((1, 4),))
    down_weight = normal_values(key_list[10], (FF, D), FF ** -0.5, 0.0625, ((0, 4),))
    mlp_gain = jnp.clip(1.0 + 0.1 * jax.random.normal(key_list[11], (D,), jnp.float32), 0.5, 1.5)
    cotangent = normal_values(key_list[12], (TOKENS, D), 1.0, 6.0, ((0, 32),), jnp.float32)
    return {"tokens": tokens, "query_weight": query_weight, "key_weight": key_weight, "value_weight": value_weight, "query_gain": query_gain, "key_gain": key_gain, "out_weight": out_weight, "attn_gain": attn_gain, "gate_weight": gate_weight, "up_weight": up_weight, "down_weight": down_weight, "mlp_gain": mlp_gain, "cotangent": cotangent}


rms_eps = 1e-06
rope_base = 500000.0

def matmul(left, right):
    return jnp.dot(left, right, preferred_element_type=jnp.float32)

def rope_tables(row_total, half_dim):
    places = (jnp.arange(row_total, dtype=jnp.int32) % L).astype(jnp.float32)
    powers = jnp.arange(half_dim, dtype=jnp.int32).astype(jnp.float32) * (2.0 / (2 * half_dim))
    frequency = jnp.exp(-math.log(rope_base) * powers)
    angles = places[:, None] * frequency[None, :]
    return (jnp.cos(angles), jnp.sin(angles))

def rotate(values, cosine_table, sine_table):
    row_total = values.shape[0]
    half_dim = cosine_table.shape[1]
    halves = values.reshape(row_total, -1, 2, half_dim)
    first_half = halves[:, :, 0, :]
    second_half = halves[:, :, 1, :]
    cosine_b = cosine_table[:, None, :]
    sine_b = sine_table[:, None, :]
    turned = jnp.stack([first_half * cosine_b - second_half * sine_b, second_half * cosine_b + first_half * sine_b], axis=2)
    return turned.reshape(row_total, -1)

def rms_scale(values):
    return lax.rsqrt(lax.optimization_barrier(jnp.mean(values * values, axis=-1, keepdims=True)) + rms_eps)

def norm_back(values, scales, gain_row, upstream):
    weighted = upstream * gain_row
    inner_mean = lax.optimization_barrier(jnp.mean(weighted * values, axis=-1, keepdims=True))
    return scales * (weighted - values * scales * scales * inner_mean)

def split_heads(array, head_count):
    return array.reshape(array.shape[0] // L, L, head_count, -1).astype(jnp.float32)

def causal_mask():
    position = jnp.arange(L, dtype=jnp.int32)
    return position[:, None] >= position[None, :]

def attend(query_rot, key_rot, value_proj, head_count):
    factor = 1.0 / math.sqrt(query_rot.shape[1] // head_count)
    scores = jnp.einsum('sqhd,skhd->shqk', split_heads(query_rot, head_count), split_heads(key_rot, head_count)) * factor
    masked = jnp.where(causal_mask(), scores, -jnp.inf)
    largest = lax.optimization_barrier(jnp.max(masked, axis=-1, keepdims=True))
    expo_vals = jnp.exp(masked - largest)
    sum_exp = lax.optimization_barrier(jnp.sum(expo_vals, axis=-1, keepdims=True))
    probability = (expo_vals / sum_exp).astype(jnp.bfloat16)
    mixed = jnp.einsum('shqk,skhd->sqhd', probability.astype(jnp.float32), split_heads(value_proj, head_count))
    return (mixed.reshape(query_rot.shape[0], -1).astype(jnp.bfloat16), largest + jnp.log(sum_exp))

def attend_back(query_rot, key_rot, value_proj, logsum, grad_attended, head_count):
    factor = 1.0 / math.sqrt(query_rot.shape[1] // head_count)
    queries = split_heads(query_rot, head_count)
    keys_all = split_heads(key_rot, head_count)
    scores = jnp.einsum('sqhd,skhd->shqk', queries, keys_all) * factor
    prob_full = jnp.exp(jnp.where(causal_mask(), scores - logsum, -jnp.inf))
    prob_low = prob_full.astype(jnp.bfloat16).astype(jnp.float32)
    grad_heads = split_heads(grad_attended, head_count)
    grad_value = jnp.einsum('shqk,sqhd->skhd', prob_low, grad_heads)
    grad_prob = jnp.einsum('sqhd,skhd->shqk', grad_heads, split_heads(value_proj, head_count))
    row_dot = lax.optimization_barrier(jnp.sum(prob_full * grad_prob, axis=-1, keepdims=True))
    grad_scores = (prob_full * (grad_prob - row_dot) * factor).astype(jnp.bfloat16).astype(jnp.float32)
    grad_query = jnp.einsum('shqk,skhd->sqhd', grad_scores, keys_all)
    grad_key = jnp.einsum('shqk,sqhd->skhd', grad_scores, queries)
    row_total = query_rot.shape[0]
    return (grad_query.reshape(row_total, -1), grad_key.reshape(row_total, -1), grad_value.reshape(row_total, -1).astype(jnp.bfloat16))

def layer_block(weights, block_tokens, block_cot):
    query_weight, key_weight, value_weight, query_gain, key_gain, out_weight, attn_gain, gate_weight, up_weight, down_weight, mlp_gain = weights
    row_total = block_tokens.shape[0]
    head_count = query_gain.shape[0]
    query_flat = query_gain.reshape(-1)
    key_flat = key_gain.reshape(-1)
    cosine_table, sine_table = rope_tables(row_total, query_gain.shape[1] // 2)
    query_proj = matmul(block_tokens, query_weight)
    key_proj = matmul(block_tokens, key_weight)
    value_proj = matmul(block_tokens, value_weight).astype(jnp.bfloat16)
    query_scale = rms_scale(query_proj)
    key_scale = rms_scale(key_proj)
    query_rot = rotate(query_proj * query_scale * query_flat, cosine_table, sine_table).astype(jnp.bfloat16)
    key_rot = rotate(key_proj * key_scale * key_flat, cosine_table, sine_table).astype(jnp.bfloat16)
    attended, logsum = attend(query_rot, key_rot, value_proj, head_count)
    attn_branch = matmul(attended, out_weight)
    attn_scale = rms_scale(attn_branch)
    hidden = block_tokens.astype(jnp.float32) + attn_branch * attn_scale * attn_gain
    hidden_low = hidden.astype(jnp.bfloat16)
    gate_proj = matmul(hidden_low, gate_weight)
    up_proj = matmul(hidden_low, up_weight)
    sigmoid_gate = jax.nn.sigmoid(gate_proj)
    swish_gate = gate_proj * sigmoid_gate
    activation = (swish_gate * up_proj).astype(jnp.bfloat16)
    mlp_branch = matmul(activation, down_weight)
    mlp_scale = rms_scale(mlp_branch)
    output = hidden + mlp_branch * mlp_scale * mlp_gain
    grad_mlp_gain = lax.optimization_barrier(jnp.sum(block_cot * mlp_branch * mlp_scale, axis=0))
    grad_mlp = norm_back(mlp_branch, mlp_scale, mlp_gain, block_cot).astype(jnp.bfloat16)
    grad_act = matmul(grad_mlp, down_weight.T)
    grad_gate = (grad_act * up_proj * sigmoid_gate * (1.0 + gate_proj * (1.0 - sigmoid_gate))).astype(jnp.bfloat16)
    grad_up = (grad_act * swish_gate).astype(jnp.bfloat16)
    grad_down_weight = matmul(activation.T, grad_mlp)
    grad_gate_weight = matmul(hidden_low.T, grad_gate)
    grad_up_weight = matmul(hidden_low.T, grad_up)
    grad_hidden = block_cot + (matmul(grad_gate, gate_weight.T) + matmul(grad_up, up_weight.T))
    grad_attn_gain = lax.optimization_barrier(jnp.sum(grad_hidden * attn_branch * attn_scale, axis=0))
    grad_branch = norm_back(attn_branch, attn_scale, attn_gain, grad_hidden).astype(jnp.bfloat16)
    grad_attended = matmul(grad_branch, out_weight.T).astype(jnp.bfloat16)
    grad_out_weight = matmul(attended.T, grad_branch)
    grad_query_rot, grad_key_rot, grad_value = attend_back(query_rot, key_rot, value_proj, logsum, grad_attended, head_count)
    grad_query_normed = rotate(grad_query_rot, cosine_table, -sine_table)
    grad_key_normed = rotate(grad_key_rot, cosine_table, -sine_table)
    grad_query_gain = lax.optimization_barrier(jnp.sum(grad_query_normed * query_proj * query_scale, axis=0)).reshape(query_gain.shape)
    grad_key_gain = lax.optimization_barrier(jnp.sum(grad_key_normed * key_proj * key_scale, axis=0)).reshape(key_gain.shape)
    grad_query = norm_back(query_proj, query_scale, query_flat, grad_query_normed).astype(jnp.bfloat16)
    grad_key = norm_back(key_proj, key_scale, key_flat, grad_key_normed).astype(jnp.bfloat16)
    grad_query_weight = matmul(block_tokens.T, grad_query)
    grad_key_weight = matmul(block_tokens.T, grad_key)
    grad_value_weight = matmul(block_tokens.T, grad_value)
    input_grad = grad_hidden + (matmul(grad_query, query_weight.T) + matmul(grad_key, key_weight.T) + matmul(grad_value, value_weight.T))
    gradients = (grad_query_weight, grad_key_weight, grad_value_weight, grad_query_gain, grad_key_gain, grad_out_weight, grad_attn_gain, grad_gate_weight, grad_up_weight, grad_down_weight, grad_mlp_gain)
    return (gradients, output, input_grad)

def reference(tokens, query_weight, key_weight, value_weight, query_gain, key_gain, out_weight, attn_gain, gate_weight, up_weight, down_weight, mlp_gain, cotangent):
    weights = (query_weight, key_weight, value_weight, query_gain, key_gain, out_weight, attn_gain, gate_weight, up_weight, down_weight, mlp_gain)
    block_rows = L * math.gcd(TOKENS // L, max(1, 4096 // L))
    block_count = TOKENS // block_rows
    starting = tuple((jnp.zeros(member.shape, jnp.float32) for member in weights))

    def block_step(carried, inputs):
        gradients, output, input_grad = layer_block(weights, inputs[0], inputs[1])
        summed = tuple((before + after for before, after in zip(carried, gradients)))
        return (summed, (output, input_grad))
    totals, results = lax.scan(block_step, starting, (tokens.reshape(block_count, block_rows, D), cotangent.reshape(block_count, block_rows, D)))
    output = results[0].reshape(TOKENS, D)
    input_grad = results[1].reshape(TOKENS, D)
    return (output, input_grad, totals[0], totals[1], totals[2], totals[3], totals[4], totals[5], totals[6], totals[7], totals[8], totals[9], totals[10])
```

```python
import functools
import math

import jax
import jax.numpy as jnp
from jax import lax
from jax.sharding import PartitionSpec as P

L = 256


rms_eps = 1e-06
rope_base = 500000.0


def matmul(left, right):
    return jnp.dot(left, right, preferred_element_type=jnp.float32)


def matmul_nt(left, right):
    return lax.dot_general(
        left, right, (((1,), (1,)), ((), ())), preferred_element_type=jnp.float32
    )


def matmul_tn(left, right):
    return lax.dot_general(
        left, right, (((0,), (0,)), ((), ())), preferred_element_type=jnp.float32
    )


def rope_tables(row_total, half_dim):
    places = (jnp.arange(row_total, dtype=jnp.int32) % L).astype(jnp.float32)
    powers = jnp.arange(half_dim, dtype=jnp.int32).astype(jnp.float32) * (2.0 / (2 * half_dim))
    frequency = jnp.exp(-math.log(rope_base) * powers)
    angles = places[:, None] * frequency[None, :]
    return (jnp.cos(angles), jnp.sin(angles))


def rotate(values, cosine_table, sine_table):
    row_total = values.shape[0]
    half_dim = cosine_table.shape[1]
    halves = values.reshape(row_total, -1, 2, half_dim)
    first_half = halves[:, :, 0, :]
    second_half = halves[:, :, 1, :]
    cosine_b = cosine_table[:, None, :]
    sine_b = sine_table[:, None, :]
    turned = jnp.stack(
        [
            first_half * cosine_b - second_half * sine_b,
            second_half * cosine_b + first_half * sine_b,
        ],
        axis=2,
    )
    return turned.reshape(row_total, -1)


def rms_scale(values):
    return lax.rsqrt(jnp.mean(values * values, axis=-1, keepdims=True) + rms_eps)


def norm_back(values, scales, gain_row, upstream):
    weighted = upstream * gain_row
    inner_mean = jnp.mean(weighted * values, axis=-1, keepdims=True)
    return scales * (weighted - values * scales * scales * inner_mean)


def split_heads(array, head_count):
    return array.reshape(array.shape[0] // L, L, head_count, -1)


def causal_mask():
    position = jnp.arange(L, dtype=jnp.int32)
    return position[:, None] >= position[None, :]


def attend(query_rot, key_rot, value_proj, head_count):
    factor = 1.0 / math.sqrt(query_rot.shape[1] // head_count)
    scores = (
        jnp.einsum(
            "sqhd,skhd->shqk",
            split_heads(query_rot, head_count),
            split_heads(key_rot, head_count),
            preferred_element_type=jnp.float32,
        )
        * factor
    )
    masked = jnp.where(causal_mask(), scores, -jnp.inf)
    largest = jnp.max(masked, axis=-1, keepdims=True)
    expo_vals = jnp.exp(masked - largest)
    sum_exp = jnp.sum(expo_vals, axis=-1, keepdims=True)
    probability = (expo_vals / sum_exp).astype(jnp.bfloat16)
    mixed = jnp.einsum(
        "shqk,skhd->sqhd",
        probability,
        split_heads(value_proj, head_count),
        preferred_element_type=jnp.float32,
    )
    return (mixed.reshape(query_rot.shape[0], -1).astype(jnp.bfloat16), largest + jnp.log(sum_exp))


def attend_back(query_rot, key_rot, value_proj, logsum, grad_attended, head_count):
    factor = 1.0 / math.sqrt(query_rot.shape[1] // head_count)
    queries = split_heads(query_rot, head_count)
    keys_all = split_heads(key_rot, head_count)
    scores = (
        jnp.einsum("sqhd,skhd->shqk", queries, keys_all, preferred_element_type=jnp.float32)
        * factor
    )
    prob_full = jnp.exp(jnp.where(causal_mask(), scores - logsum, -jnp.inf))
    prob_low = prob_full.astype(jnp.bfloat16)
    grad_heads = split_heads(grad_attended, head_count)
    grad_value = jnp.einsum(
        "shqk,sqhd->skhd", prob_low, grad_heads, preferred_element_type=jnp.float32
    )
    grad_prob = jnp.einsum(
        "sqhd,skhd->shqk",
        grad_heads,
        split_heads(value_proj, head_count),
        preferred_element_type=jnp.float32,
    )
    row_dot = jnp.sum(prob_full * grad_prob, axis=-1, keepdims=True)
    grad_scores = (prob_full * (grad_prob - row_dot) * factor).astype(jnp.bfloat16)
    grad_query = jnp.einsum(
        "shqk,skhd->sqhd", grad_scores, keys_all, preferred_element_type=jnp.float32
    )
    grad_key = jnp.einsum(
        "shqk,sqhd->skhd", grad_scores, queries, preferred_element_type=jnp.float32
    )
    row_total = query_rot.shape[0]
    return (
        grad_query.reshape(row_total, -1),
        grad_key.reshape(row_total, -1),
        grad_value.reshape(row_total, -1).astype(jnp.bfloat16),
    )


def swap_pairs(size, step):
    return [(place, place ^ step) for place in range(size)]


def owner_order(bits):
    if not bits:
        return [0]
    rest = owner_order(bits[1:])
    return [member | (1 << bits[0]) for member in rest] + rest


def half_plans(size):
    bits = list(range(1, size.bit_length() - 1))
    return bits, bits[1:] + bits[:1]


def by_owner(columns, size):
    me = lax.axis_index("dp")
    width = columns.shape[1] // size
    part = width // 2
    sent, kept = [], []
    for half, bits in enumerate(half_plans(size)):
        for mask in owner_order(bits):
            for flip, held in ((1, sent), (0, kept)):
                start = (me ^ (mask | flip)) * width + half * part
                held.append(lax.dynamic_slice_in_dim(columns, start, part, axis=1))
    return jnp.concatenate(sent, axis=1), jnp.concatenate(kept, axis=1)


def exchange(values, size, step):
    return lax.ppermute(values, "dp", swap_pairs(size, step))


def halve(values, axis, size, bits):
    for bit in bits:
        cut = values.shape[axis] // 2
        sent = lax.slice_in_dim(values, 0, cut, axis=axis).astype(jnp.bfloat16)
        arrived = exchange(sent, size, 1 << bit)
        values = lax.slice_in_dim(values, cut, 2 * cut, axis=axis) + arrived.astype(jnp.float32)
    return values


def reduce_product(product, sent, kept, axis, size):
    arrived = exchange(product(sent).astype(jnp.bfloat16), size, 1)
    held = product(kept) + arrived.astype(jnp.float32)
    cut = held.shape[axis] // 2
    first, second = half_plans(size)
    return jnp.concatenate(
        [
            halve(lax.slice_in_dim(held, 0, cut, axis=axis), axis, size, first),
            halve(lax.slice_in_dim(held, cut, 2 * cut, axis=axis), axis, size, second),
        ],
        axis=axis,
    )


def add_all(values, name, size):
    step = 1
    while step < size:
        values = values + lax.ppermute(values, name, swap_pairs(size, step))
        step *= 2
    return values


def own_part(values, axis, place, count):
    part = values.shape[axis] // count
    return lax.dynamic_slice_in_dim(values, place * part, part, axis=axis)


def scatter_low(values):
    return lax.psum_scatter(
        values.astype(jnp.bfloat16), "tensor", scatter_dimension=0, tiled=True
    ).astype(jnp.float32)


def on_device(
    dp_size,
    tensor_size,
    tokens,
    query_weight,
    key_weight,
    value_weight,
    query_gain,
    key_gain,
    out_weight,
    attn_gain,
    gate_weight,
    up_weight,
    down_weight,
    mlp_gain,
    cotangent,
):
    model_width = tokens.shape[1]
    head_count = query_gain.shape[0]
    query_flat = query_gain.reshape(-1)
    key_flat = key_gain.reshape(-1)
    gathered = lax.all_gather(tokens, "tensor", axis=0, tiled=True)
    row_total = gathered.shape[0]
    cosine_table, sine_table = rope_tables(row_total, query_gain.shape[1] // 2)
    query_proj = matmul(gathered, query_weight)
    key_proj = matmul(gathered, key_weight)
    value_proj = matmul(gathered, value_weight).astype(jnp.bfloat16)
    query_square, key_square = lax.psum(
        (jnp.sum(query_proj * query_proj, axis=-1), jnp.sum(key_proj * key_proj, axis=-1)), "tensor"
    )
    query_scale = lax.rsqrt(query_square / model_width + rms_eps)[:, None]
    key_scale = lax.rsqrt(key_square / model_width + rms_eps)[:, None]
    query_rot = rotate(query_proj * query_scale * query_flat, cosine_table, sine_table).astype(
        jnp.bfloat16
    )
    key_rot = rotate(key_proj * key_scale * key_flat, cosine_table, sine_table).astype(jnp.bfloat16)
    attended, logsum = attend(query_rot, key_rot, value_proj, head_count)
    attn_branch = scatter_low(matmul(attended, out_weight))
    attn_scale = rms_scale(attn_branch)
    hidden = tokens.astype(jnp.float32) + attn_branch * attn_scale * attn_gain
    hidden_rows = lax.all_gather(hidden.astype(jnp.bfloat16), "tensor", axis=0, tiled=True)
    gate_proj = matmul(hidden_rows, gate_weight)
    up_proj = matmul(hidden_rows, up_weight)
    sigmoid_gate = jax.nn.sigmoid(gate_proj)
    swish_gate = gate_proj * sigmoid_gate
    activation = (swish_gate * up_proj).astype(jnp.bfloat16)
    mlp_branch = scatter_low(matmul(activation, down_weight))
    mlp_scale = rms_scale(mlp_branch)
    output = hidden + mlp_branch * mlp_scale * mlp_gain
    part_mlp_gain = jnp.sum(cotangent * mlp_branch * mlp_scale, axis=0)
    grad_mlp = norm_back(mlp_branch, mlp_scale, mlp_gain, cotangent).astype(jnp.bfloat16)
    grad_mlp_rows = lax.all_gather(grad_mlp, "tensor", axis=0, tiled=True)
    grad_act = matmul_nt(grad_mlp_rows, down_weight)
    grad_gate = (
        grad_act * up_proj * sigmoid_gate * (1.0 + gate_proj * (1.0 - sigmoid_gate))
    ).astype(jnp.bfloat16)
    grad_up = (grad_act * swish_gate).astype(jnp.bfloat16)
    summed_down = reduce_product(
        lambda part: matmul_tn(activation, part), *by_owner(grad_mlp_rows, dp_size), 1, dp_size
    )
    hidden_parts = by_owner(hidden_rows, dp_size)
    summed_gate = reduce_product(
        lambda part: matmul_tn(part, grad_gate), *hidden_parts, 0, dp_size
    )
    summed_up = reduce_product(lambda part: matmul_tn(part, grad_up), *hidden_parts, 0, dp_size)
    grad_hidden = cotangent + scatter_low(
        matmul_nt(grad_gate, gate_weight) + matmul_nt(grad_up, up_weight)
    )
    part_attn_gain = jnp.sum(grad_hidden * attn_branch * attn_scale, axis=0)
    grad_branch = norm_back(attn_branch, attn_scale, attn_gain, grad_hidden).astype(jnp.bfloat16)
    grad_branch_rows = lax.all_gather(grad_branch, "tensor", axis=0, tiled=True)
    grad_attended = matmul_nt(grad_branch_rows, out_weight).astype(jnp.bfloat16)
    summed_out = reduce_product(
        lambda part: matmul_tn(attended, part), *by_owner(grad_branch_rows, dp_size), 1, dp_size
    )
    grad_query_rot, grad_key_rot, grad_value = attend_back(
        query_rot, key_rot, value_proj, logsum, grad_attended, head_count
    )
    grad_query_normed = rotate(grad_query_rot, cosine_table, -sine_table)
    grad_key_normed = rotate(grad_key_rot, cosine_table, -sine_table)
    term_query_gain = jnp.sum(grad_query_normed * query_proj * query_scale, axis=0).reshape(
        query_gain.shape
    )
    term_key_gain = jnp.sum(grad_key_normed * key_proj * key_scale, axis=0).reshape(key_gain.shape)
    query_weighted = grad_query_normed * query_flat
    key_weighted = grad_key_normed * key_flat
    query_inner, key_inner = lax.psum(
        (jnp.sum(query_weighted * query_proj, axis=-1), jnp.sum(key_weighted * key_proj, axis=-1)),
        "tensor",
    )
    grad_query = (
        query_scale
        * (
            query_weighted
            - query_proj * query_scale * query_scale * (query_inner / model_width)[:, None]
        )
    ).astype(jnp.bfloat16)
    grad_key = (
        key_scale
        * (key_weighted - key_proj * key_scale * key_scale * (key_inner / model_width)[:, None])
    ).astype(jnp.bfloat16)
    token_parts = by_owner(gathered, dp_size)
    width = grad_query.shape[1]
    grad_three = jnp.concatenate([grad_query, grad_key, grad_value], axis=1)
    summed_three = reduce_product(
        lambda part: matmul_tn(part, grad_three), *token_parts, 0, dp_size
    )
    summed_query, summed_key, summed_value = (
        summed_three[:, :width],
        summed_three[:, width : 2 * width],
        summed_three[:, 2 * width :],
    )
    input_grad = grad_hidden + scatter_low(
        matmul_nt(grad_query, query_weight)
        + matmul_nt(grad_key, key_weight)
        + matmul_nt(grad_value, value_weight)
    )
    place = lax.axis_index("dp")
    summed_gains = add_all(
        add_all(jnp.stack([part_attn_gain, part_mlp_gain]), "tensor", tensor_size), "dp", dp_size
    )
    summed_gains = own_part(
        summed_gains,
        1,
        place * tensor_size + lax.axis_index("tensor"),
        dp_size * tensor_size,
    )
    summed_attn_gain, summed_mlp_gain = summed_gains[0], summed_gains[1]
    head_gains = own_part(
        add_all(jnp.stack([term_query_gain, term_key_gain]), "dp", dp_size), 2, place, dp_size
    )
    summed_query_gain, summed_key_gain = head_gains[0], head_gains[1]
    return (
        output,
        input_grad,
        summed_query,
        summed_key,
        summed_value,
        summed_query_gain,
        summed_key_gain,
        summed_out,
        summed_attn_gain,
        summed_gate,
        summed_up,
        summed_down,
        summed_mlp_gain,
    )


def solution(mesh):
    placed = (
        P(("dp", "tensor"), None),
        P(None, "tensor"),
        P(None, "tensor"),
        P(None, "tensor"),
        P("tensor", None),
        P("tensor", None),
        P("tensor", None),
        P(),
        P(None, "tensor"),
        P(None, "tensor"),
        P("tensor", None),
        P(),
        P(("dp", "tensor"), None),
    )
    return jax.shard_map(
        functools.partial(on_device, mesh.shape["dp"], mesh.shape["tensor"]),
        mesh=mesh,
        in_specs=placed,
        out_specs=(
            P(("dp", "tensor"), None),
            P(("dp", "tensor"), None),
            P("dp", "tensor"),
            P("dp", "tensor"),
            P("dp", "tensor"),
            P("tensor", "dp"),
            P("tensor", "dp"),
            P("tensor", "dp"),
            P(("dp", "tensor")),
            P("dp", "tensor"),
            P("dp", "tensor"),
            P("tensor", "dp"),
            P(("dp", "tensor")),
        ),
        check_vma=False,
    )
```

```python
import functools
import math

import jax
import jax.numpy as jnp
from jax import lax
from jax.experimental import pallas as pl
from jax.experimental.pallas import tpu as pltpu
from jax.sharding import PartitionSpec as P

L = 256


rms_eps = 1e-06
rope_base = 500000.0


def matmul(left, right):
    return jnp.dot(left, right, preferred_element_type=jnp.float32)


def matmul_nt(left, right):
    return lax.dot_general(
        left, right, (((1,), (1,)), ((), ())), preferred_element_type=jnp.float32
    )


def matmul_tn(left, right):
    return lax.dot_general(
        left, right, (((0,), (0,)), ((), ())), preferred_element_type=jnp.float32
    )


def rope_tables(row_total, half_dim):
    places = (jnp.arange(row_total, dtype=jnp.int32) % L).astype(jnp.float32)
    powers = jnp.arange(half_dim, dtype=jnp.int32).astype(jnp.float32) * (2.0 / (2 * half_dim))
    frequency = jnp.exp(-math.log(rope_base) * powers)
    angles = places[:, None] * frequency[None, :]
    return (jnp.cos(angles), jnp.sin(angles))


def rms_scale(values):
    return lax.rsqrt(jnp.mean(values * values, axis=-1, keepdims=True) + rms_eps)


def norm_back(values, scales, gain_row, upstream):
    weighted = upstream * gain_row
    inner_mean = jnp.mean(weighted * values, axis=-1, keepdims=True)
    return scales * (weighted - values * scales * scales * inner_mean)


def swap_halves(values):
    return pltpu.roll(values, values.shape[1] // 2, 1)


def causal_scores(query_rot, key_rot):
    scores = matmul_nt(query_rot, key_rot) * (1.0 / math.sqrt(query_rot.shape[1]))
    row = lax.broadcasted_iota(jnp.int32, scores.shape, 0)
    column = lax.broadcasted_iota(jnp.int32, scores.shape, 1)
    masked = jnp.where(row >= column, scores, -jnp.inf)
    expo_vals = jnp.exp(masked - jnp.max(masked, axis=-1, keepdims=True))
    return expo_vals / jnp.sum(expo_vals, axis=-1, keepdims=True)


def attend_kernel(
    query_ref,
    key_ref,
    value_ref,
    query_scale_ref,
    key_scale_ref,
    query_gain_ref,
    key_gain_ref,
    cosine_ref,
    sine_ref,
    attended_ref,
    query_rot_ref,
    key_rot_ref,
):
    def turned(values_ref, scale_ref, gain_ref):
        normed = values_ref[...] * scale_ref[...] * gain_ref[...]
        return (normed * cosine_ref[...] + swap_halves(normed) * sine_ref[...]).astype(jnp.bfloat16)

    query_rot = turned(query_ref, query_scale_ref, query_gain_ref)
    key_rot = turned(key_ref, key_scale_ref, key_gain_ref)
    probability = causal_scores(query_rot, key_rot).astype(jnp.bfloat16)
    attended_ref[...] = matmul(probability, value_ref[...]).astype(jnp.bfloat16)
    query_rot_ref[...] = query_rot
    key_rot_ref[...] = key_rot


def attend_back_kernel(
    upstream_ref,
    query_rot_ref,
    key_rot_ref,
    value_ref,
    query_ref,
    key_ref,
    query_scale_ref,
    key_scale_ref,
    query_gain_ref,
    key_gain_ref,
    cosine_ref,
    sine_ref,
    grad_query_ref,
    grad_key_ref,
    grad_value_ref,
    query_inner_ref,
    key_inner_ref,
    query_term_ref,
    key_term_ref,
):
    query_rot, key_rot, upstream = query_rot_ref[...], key_rot_ref[...], upstream_ref[...]
    prob_full = causal_scores(query_rot, key_rot)
    grad_value_ref[...] = matmul_tn(prob_full.astype(jnp.bfloat16), upstream).astype(jnp.bfloat16)
    grad_prob = matmul_nt(upstream, value_ref[...])
    row_dot = jnp.sum(prob_full * grad_prob, axis=-1, keepdims=True)
    factor = 1.0 / math.sqrt(query_rot.shape[1])
    grad_scores = (prob_full * (grad_prob - row_dot) * factor).astype(jnp.bfloat16)

    def back(grad_rot, values_ref, scale_ref, gain_ref, grad_ref, inner_ref, term_ref):
        grad_normed = grad_rot * cosine_ref[...] - swap_halves(grad_rot) * sine_ref[...]
        values = values_ref[...]
        weighted = grad_normed * gain_ref[...]
        grad_ref[...] = weighted
        term_ref[0] = jnp.sum(grad_normed * values * scale_ref[...], axis=0, keepdims=True)
        inner = jnp.sum(weighted * values, axis=-1, keepdims=True)

        @pl.when(pl.program_id(1) == 0)
        def _():
            inner_ref[...] = inner

        @pl.when(pl.program_id(1) > 0)
        def _():
            inner_ref[...] += inner

    back(
        matmul(grad_scores, key_rot),
        query_ref,
        query_scale_ref,
        query_gain_ref,
        grad_query_ref,
        query_inner_ref,
        query_term_ref,
    )
    back(
        matmul_tn(grad_scores, query_rot),
        key_ref,
        key_scale_ref,
        key_gain_ref,
        grad_key_ref,
        key_inner_ref,
        key_term_ref,
    )


def head_call(kernel, ins, out_shapes, head_dim):
    row_total, width = ins[0].shape
    grid = (row_total // L, width // head_dim)

    def spec(shape):
        if len(shape) == 3:
            return pl.BlockSpec((1, 1, head_dim), lambda s, h: (s, 0, h))
        if shape[0] == row_total and shape[1] == width:
            return pl.BlockSpec((L, head_dim), lambda s, h: (s, h))
        if shape[0] == row_total:
            return pl.BlockSpec((L, 1), lambda s, h: (s, 0))
        if shape[0] == 1:
            return pl.BlockSpec((1, head_dim), lambda s, h: (0, h))
        return pl.BlockSpec((L, head_dim), lambda s, h: (0, 0))

    return pl.pallas_call(
        kernel,
        grid=grid,
        out_shape=out_shapes,
        in_specs=[spec(member.shape) for member in ins],
        out_specs=[spec(member.shape) for member in out_shapes],
        cost_estimate=pl.CostEstimate(
            flops=8 * row_total * L * width, bytes_accessed=16 * row_total * width, transcendentals=0
        ),
    )(*ins)


def pick_kernel(part, order_ref, source_ref, target_ref):
    for place in range(target_ref.shape[1] // part):
        start = pl.multiple_of(order_ref[place] * part, part)
        target_ref[:, place * part : (place + 1) * part] = source_ref[:, pl.ds(start, part)]


def pick_blocks(columns, order, part):
    count = len(order)
    if part % 128:
        return jnp.concatenate(
            [lax.dynamic_slice_in_dim(columns, place * part, part, axis=1) for place in order],
            axis=1,
        )
    whole = pl.BlockSpec(memory_space=pltpu.VMEM)
    return pl.pallas_call(
        functools.partial(pick_kernel, part),
        in_specs=[pl.BlockSpec(memory_space=pltpu.SMEM), whole],
        out_specs=whole,
        out_shape=jax.ShapeDtypeStruct((columns.shape[0], count * part), columns.dtype),
        cost_estimate=pl.CostEstimate(
            flops=0, bytes_accessed=4 * columns.size, transcendentals=0
        ),
    )(jnp.stack(order), columns)


def swap_pairs(size, step):
    return [(place, place ^ step) for place in range(size)]


def owner_order(bits):
    if not bits:
        return [0]
    rest = owner_order(bits[1:])
    return [member | (1 << bits[0]) for member in rest] + rest


def half_plans(size):
    bits = list(range(1, size.bit_length() - 1))
    return bits, bits[1:] + bits[:1]


def by_owner(columns, size):
    me = lax.axis_index("dp")
    part = columns.shape[1] // size // 2
    order = [
        (me ^ (mask | flip)) * 2 + half
        for flip in (1, 0)
        for half, bits in enumerate(half_plans(size))
        for mask in owner_order(bits)
    ]
    picked = pick_blocks(columns, order, part)
    cut = columns.shape[1] // 2
    return picked[:, :cut], picked[:, cut:]


def exchange(values, size, step):
    return lax.ppermute(values, "dp", swap_pairs(size, step))


def halve(values, axis, size, bits):
    for bit in bits:
        cut = values.shape[axis] // 2
        sent = lax.slice_in_dim(values, 0, cut, axis=axis).astype(jnp.bfloat16)
        arrived = exchange(sent, size, 1 << bit)
        values = lax.slice_in_dim(values, cut, 2 * cut, axis=axis) + arrived.astype(jnp.float32)
    return values


def reduce_product(product, sent, kept, axis, size):
    arrived = exchange(product(sent).astype(jnp.bfloat16), size, 1)
    held = product(kept) + arrived.astype(jnp.float32)
    cut = held.shape[axis] // 2
    first, second = half_plans(size)
    return jnp.concatenate(
        [
            halve(lax.slice_in_dim(held, 0, cut, axis=axis), axis, size, first),
            halve(lax.slice_in_dim(held, cut, 2 * cut, axis=axis), axis, size, second),
        ],
        axis=axis,
    )


def add_all(values, name, size):
    step = 1
    while step < size:
        values = values + lax.ppermute(values, name, swap_pairs(size, step))
        step *= 2
    return values


def own_part(values, axis, place, count):
    part = values.shape[axis] // count
    return lax.dynamic_slice_in_dim(values, place * part, part, axis=axis)


STEPS = 8
LINE_COST = 3000


def line_kernel(size, steps, summed, spread, middle, in_count, out_count, *refs):
    me = lax.axis_index("tensor")
    first_ref = refs[0]
    ins = refs[1:in_count]
    outs = refs[in_count : in_count + out_count]
    scratch = list(refs[in_count + out_count :])
    all_rows = (first_ref if summed else outs[0]).shape[0]
    block = all_rows // size
    part = block // steps
    if summed:
        right_ref, left_ref, sum_sent, sum_come = scratch[:4]
        del scratch[:4]
    if spread:
        spread_sent, spread_come = scratch

    def rows(owner, chunk):
        return pl.ds(pl.multiple_of(owner * block + chunk * part, part), part)

    def mine(chunk):
        return pl.ds(pl.multiple_of(chunk * part, part), part)

    has_left, has_right = me > 0, me < size - 1
    right, left = jnp.minimum(me + 1, size - 1), jnp.maximum(me - 1, 0)

    barrier = pltpu.get_barrier_semaphore()

    @pl.when(has_left)
    def _():
        pl.semaphore_signal(
            barrier, inc=1, device_id={"tensor": left}, device_id_type=pl.DeviceIdType.MESH
        )

    @pl.when(has_right)
    def _():
        pl.semaphore_signal(
            barrier, inc=1, device_id={"tensor": right}, device_id_type=pl.DeviceIdType.MESH
        )

    pl.semaphore_wait(barrier, has_left.astype(jnp.int32) + has_right.astype(jnp.int32))

    def move(source, target, sent, come, device):
        return pltpu.make_async_remote_copy(
            src_ref=source,
            dst_ref=target,
            send_sem=sent,
            recv_sem=come,
            device_id={"tensor": device},
            device_id_type=pl.DeviceIdType.MESH,
        )

    def sum_copy(way, owner, chunk):
        held = (right_ref, left_ref)[way]
        place = held.at[rows(owner, chunk)]
        return move(
            place,
            place,
            sum_sent.at[way, owner, chunk],
            sum_come.at[way, owner, chunk],
            (right, left)[way],
        )

    def spread_copy(way, owner, chunk):
        place = outs[0].at[rows(owner, chunk)]
        return move(
            place,
            place,
            spread_sent.at[way, owner, chunk],
            spread_come.at[owner, chunk],
            (right, left)[way],
        )

    def sum_step(distance, chunk):
        for way in (0, 1):
            owner = me + distance if way == 0 else me - distance
            inside = owner < size if way == 0 else owner >= 0
            behind = has_left if way == 0 else has_right

            @pl.when(inside)
            def _(way=way, owner=owner, behind=behind):
                held = (right_ref, left_ref)[way]
                place = rows(owner, chunk)

                @pl.when(behind)
                def _():
                    sum_copy(way, owner, chunk).wait_recv()
                    held[place] = (
                        held[place].astype(jnp.float32) + first_ref[place].astype(jnp.float32)
                    ).astype(held.dtype)

                @pl.when(jnp.logical_not(behind))
                def _():
                    held[place] = first_ref[place].astype(held.dtype)

                sum_copy(way, owner, chunk).start()

    def middle_step(chunk):
        place = rows(me, chunk)
        if summed:
            for way, behind in ((0, has_left), (1, has_right)):
                held = (right_ref, left_ref)[way]

                @pl.when(behind)
                def _(way=way):
                    sum_copy(way, me, chunk).wait_recv()

                @pl.when(jnp.logical_not(behind))
                def _(held=held):
                    held[place] = jnp.zeros((part, held.shape[1]), held.dtype)

            total = first_ref[place].astype(jnp.float32) + (
                right_ref[place].astype(jnp.float32) + left_ref[place].astype(jnp.float32)
            )
        else:
            total = first_ref[mine(chunk)]
        result = middle(total, mine(chunk), ins, outs, chunk)
        if spread:
            outs[0][place] = result.astype(outs[0].dtype)

            @pl.when(has_right)
            def _():
                spread_copy(0, me, chunk).start()

            @pl.when(has_left)
            def _():
                spread_copy(1, me, chunk).start()

    def pass_step(distance, chunk):
        @pl.when(me - distance >= 0)
        def _():
            spread_copy(0, me - distance, chunk).wait_recv()

            @pl.when(has_right)
            def _():
                spread_copy(0, me - distance, chunk).start()

        @pl.when(me + distance < size)
        def _():
            spread_copy(1, me + distance, chunk).wait_recv()

            @pl.when(has_left)
            def _():
                spread_copy(1, me + distance, chunk).start()

    def at(step, lag, action):
        chunk = step - lag

        @pl.when((chunk >= 0) & (chunk < steps))
        def _():
            action(chunk)

    lag = size - 1 if summed else 0

    def step_body(step, carry):
        if summed:
            for distance in range(size - 1, 0, -1):
                at(step, size - 1 - distance, functools.partial(sum_step, distance))
        at(step, lag, middle_step)
        if spread:
            for distance in range(1, size):
                at(step, lag + distance, functools.partial(pass_step, distance))
        return carry

    lax.fori_loop(0, steps + lag + (size - 1 if spread else 0), step_body, 0)

    def drain(chunk, carry):
        for distance in range(size):
            if summed and distance > 0:

                @pl.when(me + distance < size)
                def _(distance=distance):
                    sum_copy(0, me + distance, chunk).wait_send()

                @pl.when(me - distance >= 0)
                def _(distance=distance):
                    sum_copy(1, me - distance, chunk).wait_send()

            if spread:

                @pl.when((me - distance >= 0) & has_right)
                def _(distance=distance):
                    spread_copy(0, me - distance, chunk).wait_send()

                @pl.when((me + distance < size) & has_left)
                def _(distance=distance):
                    spread_copy(1, me + distance, chunk).wait_send()

        return carry

    lax.fori_loop(0, steps, drain, 0)


def on_line(size, number, summed, spread, middle, first, ins, out_shapes, steps=STEPS):
    width = first.shape[1]
    all_rows = first.shape[0] if summed else first.shape[0] * size
    scratch = []
    if summed:
        scratch += [
            pltpu.VMEM((all_rows, width), jnp.bfloat16),
            pltpu.VMEM((all_rows, width), jnp.bfloat16),
            pltpu.SemaphoreType.DMA((2, size, steps)),
            pltpu.SemaphoreType.DMA((2, size, steps)),
        ]
    if spread:
        scratch += [
            pltpu.SemaphoreType.DMA((2, size, steps)),
            pltpu.SemaphoreType.DMA((size, steps)),
        ]
        out_shapes = [jax.ShapeDtypeStruct((all_rows, width), jnp.bfloat16)] + list(out_shapes)
    whole = pl.BlockSpec(memory_space=pltpu.VMEM)
    return pl.pallas_call(
        functools.partial(
            line_kernel, size, steps, summed, spread, middle, 1 + len(ins), len(out_shapes)
        ),
        out_shape=out_shapes,
        in_specs=[whole] * (1 + len(ins)),
        out_specs=[whole] * len(out_shapes),
        scratch_shapes=scratch,
        compiler_params=pltpu.CompilerParams(
            collective_id=number, has_side_effects=True, vmem_limit_bytes=40 * 1024 * 1024
        ),
        cost_estimate=pl.CostEstimate(
            flops=LINE_COST * (int(summed) + int(spread)) * all_rows * width,
            bytes_accessed=4 * all_rows * width,
            transcendentals=0,
        ),
    )(first, *ins)


def low(shape):
    return jax.ShapeDtypeStruct(shape, jnp.bfloat16)


def full(shape):
    return jax.ShapeDtypeStruct(shape, jnp.float32)


def middle_gather(total, place, ins, outs, chunk):
    return total


def middle_sum(total, place, ins, outs, chunk):
    outs[0][place] = total


def middle_hidden(branch, place, ins, outs, chunk):
    tokens_ref, gain_ref = ins
    _, branch_ref, hidden_ref = outs
    hidden = tokens_ref[place].astype(jnp.float32) + branch * rms_scale(branch) * gain_ref[...]
    branch_ref[place] = branch
    hidden_ref[place] = hidden
    return hidden


def add_row(gain_ref, values, chunk):
    row = jnp.sum(values, axis=0, keepdims=True)

    @pl.when(chunk == 0)
    def _():
        gain_ref[...] = row

    @pl.when(chunk > 0)
    def _():
        gain_ref[...] += row


def middle_output(branch, place, ins, outs, chunk):
    hidden_ref, cotangent_ref, gain_ref = ins
    _, output_ref, part_ref = outs
    scale = rms_scale(branch)
    scaled = branch * scale
    cotangent = cotangent_ref[place]
    output_ref[place] = hidden_ref[place] + scaled * gain_ref[...]
    add_row(part_ref, cotangent * scaled, chunk)
    return norm_back(branch, scale, gain_ref[...], cotangent)


def middle_branch(total, place, ins, outs, chunk):
    cotangent_ref, branch_ref, gain_ref = ins
    _, grad_ref, part_ref = outs
    branch = branch_ref[place]
    scale = rms_scale(branch)
    grad_hidden = cotangent_ref[place] + total
    grad_ref[place] = grad_hidden
    add_row(part_ref, grad_hidden * branch * scale, chunk)
    return norm_back(branch, scale, gain_ref[...], grad_hidden)


def on_device(
    dp_size,
    tensor_size,
    tokens,
    query_weight,
    key_weight,
    value_weight,
    query_gain,
    key_gain,
    out_weight,
    attn_gain,
    gate_weight,
    up_weight,
    down_weight,
    mlp_gain,
    cotangent,
):
    model_width = tokens.shape[1]
    query_flat = query_gain.reshape(-1)
    key_flat = key_gain.reshape(-1)
    attn_row, mlp_row = attn_gain[None, :], mlp_gain[None, :]
    own_rows = tokens.shape
    on = functools.partial(on_line, tensor_size)
    (gathered,) = on(0, False, True, middle_gather, tokens, (), ())
    row_total = gathered.shape[0]
    head_dim = query_gain.shape[1]
    query_row, key_row = query_flat[None, :], key_flat[None, :]
    cosine_half, sine_half = rope_tables(L, head_dim // 2)
    cosine_table = jnp.concatenate([cosine_half, cosine_half], axis=1)
    sine_table = jnp.concatenate([-sine_half, sine_half], axis=1)
    query_proj = matmul(gathered, query_weight)
    key_proj = matmul(gathered, key_weight)
    value_proj = matmul(gathered, value_weight).astype(jnp.bfloat16)
    query_square, key_square = lax.psum(
        (jnp.sum(query_proj * query_proj, axis=-1), jnp.sum(key_proj * key_proj, axis=-1)), "tensor"
    )
    query_scale = lax.rsqrt(query_square / model_width + rms_eps)[:, None]
    key_scale = lax.rsqrt(key_square / model_width + rms_eps)[:, None]
    attended, query_rot, key_rot = head_call(
        attend_kernel,
        (
            query_proj,
            key_proj,
            value_proj,
            query_scale,
            key_scale,
            query_row,
            key_row,
            cosine_table,
            sine_table,
        ),
        [low(value_proj.shape)] * 3,
        head_dim,
    )
    hidden_rows, attn_branch, hidden = on(
        1,
        True,
        True,
        middle_hidden,
        matmul(attended, out_weight),
        (tokens, attn_row),
        (full(own_rows), full(own_rows)),
    )
    gate_proj = matmul(hidden_rows, gate_weight)
    up_proj = matmul(hidden_rows, up_weight)
    sigmoid_gate = jax.nn.sigmoid(gate_proj)
    swish_gate = gate_proj * sigmoid_gate
    activation = (swish_gate * up_proj).astype(jnp.bfloat16)
    grad_mlp_rows, output, part_mlp_gain = on(
        2,
        True,
        True,
        middle_output,
        matmul(activation, down_weight),
        (hidden, cotangent, mlp_row),
        (full(own_rows), full(mlp_row.shape)),
    )
    grad_act = matmul_nt(grad_mlp_rows, down_weight)
    grad_gate = (
        grad_act * up_proj * sigmoid_gate * (1.0 + gate_proj * (1.0 - sigmoid_gate))
    ).astype(jnp.bfloat16)
    grad_up = (grad_act * swish_gate).astype(jnp.bfloat16)
    summed_down = reduce_product(
        lambda part: matmul_tn(activation, part), *by_owner(grad_mlp_rows, dp_size), 1, dp_size
    )
    hidden_parts = by_owner(hidden_rows, dp_size)
    summed_gate = reduce_product(
        lambda part: matmul_tn(part, grad_gate), *hidden_parts, 0, dp_size
    )
    summed_up = reduce_product(lambda part: matmul_tn(part, grad_up), *hidden_parts, 0, dp_size)
    grad_branch_rows, grad_hidden, part_attn_gain = on(
        3,
        True,
        True,
        middle_branch,
        matmul_nt(grad_gate, gate_weight) + matmul_nt(grad_up, up_weight),
        (cotangent, attn_branch, attn_row),
        (full(own_rows), full(attn_row.shape)),
    )
    grad_attended = matmul_nt(grad_branch_rows, out_weight).astype(jnp.bfloat16)
    summed_out = reduce_product(
        lambda part: matmul_tn(attended, part), *by_owner(grad_branch_rows, dp_size), 1, dp_size
    )
    row_total = gathered.shape[0]
    terms_shape = (row_total // L, 1, query_flat.shape[0])
    query_weighted, key_weighted, grad_value, query_part, key_part, query_terms, key_terms = head_call(
        attend_back_kernel,
        (
            grad_attended,
            query_rot,
            key_rot,
            value_proj,
            query_proj,
            key_proj,
            query_scale,
            key_scale,
            query_row,
            key_row,
            cosine_table,
            sine_table,
        ),
        [
            full(query_proj.shape),
            full(query_proj.shape),
            low(query_proj.shape),
            full((row_total, 1)),
            full((row_total, 1)),
            full(terms_shape),
            full(terms_shape),
        ],
        head_dim,
    )
    term_query_gain = jnp.sum(query_terms, axis=0).reshape(query_gain.shape)
    term_key_gain = jnp.sum(key_terms, axis=0).reshape(key_gain.shape)
    query_inner, key_inner = lax.psum((query_part[:, 0], key_part[:, 0]), "tensor")
    grad_query = (
        query_scale
        * (
            query_weighted
            - query_proj * query_scale * query_scale * (query_inner / model_width)[:, None]
        )
    ).astype(jnp.bfloat16)
    grad_key = (
        key_scale
        * (key_weighted - key_proj * key_scale * key_scale * (key_inner / model_width)[:, None])
    ).astype(jnp.bfloat16)
    token_parts = by_owner(gathered, dp_size)
    width = grad_query.shape[1]
    grad_three = jnp.concatenate([grad_query, grad_key, grad_value], axis=1)
    summed_three = reduce_product(
        lambda part: matmul_tn(part, grad_three), *token_parts, 0, dp_size
    )
    summed_query, summed_key, summed_value = (
        summed_three[:, :width],
        summed_three[:, width : 2 * width],
        summed_three[:, 2 * width :],
    )
    (input_sum,) = on(
        4,
        True,
        False,
        middle_sum,
        matmul_nt(grad_query, query_weight)
        + matmul_nt(grad_key, key_weight)
        + matmul_nt(grad_value, value_weight),
        (),
        (full(own_rows),),
    )
    input_grad = grad_hidden + input_sum
    place = lax.axis_index("dp")
    summed_gains = add_all(
        add_all(jnp.concatenate([part_attn_gain, part_mlp_gain]), "tensor", tensor_size), "dp", dp_size
    )
    summed_gains = own_part(
        summed_gains,
        1,
        place * tensor_size + lax.axis_index("tensor"),
        dp_size * tensor_size,
    )
    summed_attn_gain, summed_mlp_gain = summed_gains[0], summed_gains[1]
    head_gains = own_part(
        add_all(jnp.stack([term_query_gain, term_key_gain]), "dp", dp_size), 2, place, dp_size
    )
    summed_query_gain, summed_key_gain = head_gains[0], head_gains[1]
    return (
        output,
        input_grad,
        summed_query,
        summed_key,
        summed_value,
        summed_query_gain,
        summed_key_gain,
        summed_out,
        summed_attn_gain,
        summed_gate,
        summed_up,
        summed_down,
        summed_mlp_gain,
    )


def solution(mesh):
    placed = (
        P(("dp", "tensor"), None),
        P(None, "tensor"),
        P(None, "tensor"),
        P(None, "tensor"),
        P("tensor", None),
        P("tensor", None),
        P("tensor", None),
        P(),
        P(None, "tensor"),
        P(None, "tensor"),
        P("tensor", None),
        P(),
        P(("dp", "tensor"), None),
    )
    return jax.shard_map(
        functools.partial(on_device, mesh.shape["dp"], mesh.shape["tensor"]),
        mesh=mesh,
        in_specs=placed,
        out_specs=(
            P(("dp", "tensor"), None),
            P(("dp", "tensor"), None),
            P("dp", "tensor"),
            P("dp", "tensor"),
            P("dp", "tensor"),
            P("tensor", "dp"),
            P("tensor", "dp"),
            P("tensor", "dp"),
            P(("dp", "tensor")),
            P("dp", "tensor"),
            P("dp", "tensor"),
            P("tensor", "dp"),
            P(("dp", "tensor")),
        ),
        check_vma=False,
    )
```
